256 devices in a mesh: elem: 32 (over y_lo, z, core), test: 8 (over y_hi, x).
Axes of the slice: x: 4, y: 4 (y_hi: 2, y_lo: 2; y = y_hi * 2 + y_lo), z: 8, core: 2. Of those that a mesh axis runs over, the one named last changes fastest.
Arguments:
- mode_fields: bfloat16 [64, 3, 131072], P('test', None, 'elem'), may hold values from -6 to 6
- elem_type: int32 [256], P('elem'), may hold values from 0 to 3
- type_scales: float32 [4, 3], replicated, may hold values from 0.5 to 2
Outputs:
- conv_tensor: float32 [64, 64, 64], P('test', 'elem')
The draws below stay inside these ranges and needn't reach their ends.
All inputs are finite; a program needn't handle non-finite values.
Results may differ from the reference program's by a relative error of at most 0.0051.
Values may be sent and summed in bfloat16 or wider, within the bound.
No kernel may reach another device: no remote copies, remote signals or barrier semaphores. Data moves between devices by JAX's collectives and lax.ppermute only.
A program may use at most 64 MiB of HBM per device.

```python
import math
import jax
import jax.numpy as jnp
import numpy as np
from jax import lax

M = 64
Q = 8
TYPES = 4
NELEM = 256
NPTS = 131072
N_ELEM = 32
N_TEST = 8


def set_ends(values, key, low, top_value):
    place = [jax.random.randint(jax.random.fold_in(key, axis), (), 0, length) for axis, length in enumerate(values.shape)]
    widest = values.shape.index(max(values.shape))
    beside = place[:widest] + [(place[widest] + 1) % values.shape[widest]] + place[widest + 1:]
    return values.at[tuple(place)].set(low).at[tuple(beside)].set(top_value)


def block_scale(key, dims, split, smallest, high):
    factor_of = 1.0
    for axis_at, blocks in split:
        heights = jax.random.uniform(jax.random.fold_in(jax.random.fold_in(key, 6), axis_at), (blocks,), jnp.float32, smallest / len(split), high / len(split))
        factor_of = factor_of * jnp.repeat(jnp.exp(heights), dims[axis_at] // blocks).reshape((-1,) + (1,) * (len(dims) - 1 - axis_at))
    return factor_of


def bell_draw(own_key, shape, spread, most, split=(), held_as=jnp.bfloat16):
    factor_of = block_scale(own_key, shape, split, -0.22, 0.18) if split else 1.0
    values = jax.random.normal(own_key, shape, jnp.float32) * spread * factor_of
    return jnp.minimum(jnp.maximum(values, -most), most).astype(held_as)


def setup_inputs(seed: int = 0) -> dict:
    streams_of = jax.random.split(jax.random.key(seed), 4)
    return {
        "mode_fields": bell_draw(streams_of[0], (M, 3, NPTS), 1.0, 6.0, ((0, 8), (2, 32))),
        "elem_type": set_ends(jax.random.randint(streams_of[1], (NELEM,), 0, TYPES), jax.random.fold_in(streams_of[1], 1), 0, TYPES - 1).astype(jnp.int32),
        "type_scales": jnp.clip(jnp.exp(jax.random.uniform(streams_of[2], (TYPES, 3), jnp.float32, math.log(0.5), math.log(2.0))), 0.5, 2.0),
    }


block_modes = 4


def legendre_top(points, degree):
    before = points * 0.0 + 1.0
    current = points
    for order in range(2, degree + 1):
        following = ((2 * order - 1) * points * current - (order - 1) * before) / order
        before = current
        current = following
    return current, before


def lobatto_tables(order_points):
    degree = order_points - 1
    lobatto_nodes = np.cos(np.pi * np.arange(degree + 1) / degree)
    for sweep in range(100):
        top, lower = legendre_top(lobatto_nodes, degree)
        lobatto_nodes = lobatto_nodes - (lobatto_nodes * top - lower) / ((degree + 1) * top)
    lobatto_nodes = lobatto_nodes[::-1].copy()
    lobatto_nodes[0] = -1.0
    lobatto_nodes[-1] = 1.0
    values, unused = legendre_top(lobatto_nodes, degree)
    weights = 2.0 / (degree * (degree + 1) * values ** 2)
    identity = np.eye(order_points)
    distance = lobatto_nodes[:, None] - lobatto_nodes[None, :]
    spacing = np.where(identity > 0, 1.0, distance)
    derivative = np.where(identity > 0, 0.0, values[:, None] / values[None, :] / spacing)
    corner = degree * (degree + 1) / 4.0
    ends = np.concatenate([[-corner], np.zeros(degree - 1), [corner]])
    derivative = derivative + identity * ends[None, :]
    square_eye = np.eye(order_points * order_points)
    along_r = np.kron(square_eye, derivative)
    along_s = np.kron(identity, np.kron(derivative, identity))
    along_t = np.kron(derivative, square_eye)
    table = np.concatenate([along_r.T, along_s.T, along_t.T], axis=1)
    cube_weights = np.kron(weights, np.kron(weights, weights))
    return table.astype(np.float32), cube_weights.astype(np.float32)


def element_scales(types, type_scales):
    picks = (types[:, None] == jnp.arange(type_scales.shape[0], dtype=jnp.int32)[None, :]).astype(jnp.float32)
    return jnp.sum(picks[:, :, None] * type_scales[None, :, :], axis=1)


def gradient(fields, scales, table, cube):
    mode_count = fields.shape[0]
    elements = fields.shape[2] // cube
    flat = fields.reshape(mode_count * 3 * elements, cube)
    derived = jnp.dot(flat, table, preferred_element_type=jnp.float32).reshape(mode_count, 3, elements, 3, cube)
    return (derived * scales[None, None, :, :, None]).astype(jnp.bfloat16)


def project(test_fields, trial_fields, grads, quadrature):
    test_modes = test_fields.shape[0]
    trial_modes = trial_fields.shape[0]
    grad_modes = grads.shape[0]
    blocks = grads.reshape((grad_modes // block_modes, block_modes) + grads.shape[1:])
    test_wide = test_fields.astype(jnp.float32)
    trial_wide = trial_fields.astype(jnp.float32)

    def one_block(grad_block):
        grad_wide = grad_block.astype(jnp.float32)
        summed = test_wide[:, None, 0, :, None, :] * grad_wide[None, :, 0]
        summed = summed + test_wide[:, None, 1, :, None, :] * grad_wide[None, :, 1]
        summed = summed + test_wide[:, None, 2, :, None, :] * grad_wide[None, :, 2]
        pairs = (summed * quadrature[None, None, :, None, :]).astype(jnp.bfloat16)
        return jnp.einsum('ikedp,jdep->ijk', pairs.astype(jnp.float32), trial_wide)

    result = lax.map(one_block, blocks)
    return result.transpose(1, 2, 0, 3).reshape(test_modes, trial_modes, grad_modes)


def reference(mode_fields, elem_type, type_scales):
    table, cube_weights = lobatto_tables(Q)
    table = jnp.asarray(table).astype(jnp.bfloat16)
    point_weights = jnp.asarray(cube_weights).astype(jnp.float32)
    cube = Q ** 3
    nblocks = N_ELEM * N_TEST
    per_block = NELEM // nblocks

    def step(total, inputs):
        index, types_block = inputs
        start = (index * (per_block * cube)).astype(jnp.int32)
        block = lax.dynamic_slice_in_dim(mode_fields, start, per_block * cube, 2)
        scales = element_scales(types_block, type_scales)
        quadrature = point_weights[None, :] / jnp.prod(scales, axis=1)[:, None]
        grads = gradient(block, scales, table, cube)
        shaped = block.reshape(M, 3, per_block, cube)
        return total + project(shaped, shaped, grads, quadrature), None

    total, _ = lax.scan(step, jnp.zeros((M, M, M), jnp.float32),
                        (jnp.arange(nblocks, dtype=jnp.int32), elem_type.reshape(nblocks, per_block)))
    return total * (float(NPTS) ** -0.5)
```

```python
import functools

import jax
import jax.numpy as jnp
import numpy as np
from jax import lax
from jax.experimental import pallas as pl
from jax.experimental.pallas import tpu as pltpu
from jax.sharding import Mesh, PartitionSpec as P

Q = 8
CUBE = Q**3
MODES = 64
LANES = 128
OWNERS = 16


def legendre_top(points, degree):
    before = points * 0.0 + 1.0
    current = points
    for order in range(2, degree + 1):
        following = ((2 * order - 1) * points * current - (order - 1) * before) / order
        before = current
        current = following
    return (current, before)


def lobatto_tables(order_points):
    degree = order_points - 1
    lobatto_nodes = np.cos(np.pi * np.arange(degree + 1) / degree)
    for sweep in range(100):
        top, lower = legendre_top(lobatto_nodes, degree)
        lobatto_nodes = lobatto_nodes - (lobatto_nodes * top - lower) / ((degree + 1) * top)
    lobatto_nodes = lobatto_nodes[::-1].copy()
    lobatto_nodes[0] = -1.0
    lobatto_nodes[-1] = 1.0
    values, unused = legendre_top(lobatto_nodes, degree)
    weights = 2.0 / (degree * (degree + 1) * values**2)
    identity = np.eye(order_points)
    distance = lobatto_nodes[:, None] - lobatto_nodes[None, :]
    spacing = np.where(identity > 0, 1.0, distance)
    derivative = np.where(identity > 0, 0.0, values[:, None] / values[None, :] / spacing)
    corner = degree * (degree + 1) / 4.0
    ends = np.concatenate([[-corner], np.zeros(degree - 1), [corner]])
    derivative = derivative + identity * ends[None, :]
    block_r = np.kron(np.eye(16), derivative)
    block_s = np.kron(np.eye(2), np.kron(derivative, identity))
    block_rs = np.concatenate([block_r.T, block_s.T], axis=1)
    along_t = np.kron(derivative, np.eye(order_points * order_points))
    cube_weights = np.kron(weights, np.kron(weights, weights))
    return (
        block_rs.astype(np.float32),
        along_t.T.astype(np.float32),
        cube_weights.astype(np.float32),
    )


def tensor_kernel(core_ref, x_ref, wq_ref, rs_ref, tt_ref, send_ref, own_ref, wide, grads, tests, prods):
    bf16 = jnp.bfloat16
    narrow = []
    high = (lax.broadcasted_iota(jnp.int32, (MODES, CUBE), 0) & 2) != 0
    swap = jnp.broadcast_to(core_ref[0], (MODES, CUBE)) != 0
    for c in range(3):
        rows = jnp.concatenate([x_ref[s, c].astype(jnp.float32) for s in range(8)], axis=0)
        turned = jnp.where(high, pltpu.roll(rows, 2, 0), pltpu.roll(rows, MODES - 2, 0))
        wide[c] = jnp.where(swap, turned, rows)
        narrow.append(rows.astype(bf16))
        tests[:, c * CUBE : (c + 1) * CUBE] = narrow[c]
    panel = jnp.concatenate(narrow, axis=0)
    along_t = jnp.dot(panel, tt_ref[...], preferred_element_type=jnp.float32)
    for b in range(CUBE // LANES):
        at = slice(b * LANES, (b + 1) * LANES)
        along_rs = jnp.dot(panel[:, at], rs_ref[...], preferred_element_type=jnp.float32)
        parts = (along_rs[:, :LANES], along_rs[:, LANES:], along_t[:, at])
        for d in range(3):
            scaled = (parts[d] * wq_ref[d : d + 1, at]).astype(bf16)
            for c in range(3):
                grads[c, d, :, at] = scaled[c * MODES : (c + 1) * MODES]
    for slot, out_ref in ((0, send_ref), (1, own_ref)):
        for pair in range(OWNERS // 2):
            hold = prods.at[pair % 2]
            trial = [
                4 * (2 * pair + a) + 2 * (1 - slot) + jj for a in range(2) for jj in range(2)
            ]
            for b in range(CUBE // LANES):
                at = slice(b * LANES, (b + 1) * LANES)
                fields = [
                    [
                        jnp.broadcast_to(wide[d, j : j + 1, at], (16, LANES)).astype(bf16)
                        for d in range(3)
                    ]
                    for j in trial
                ]
                for k in range(MODES // 16):
                    rows = slice(k * 16, (k + 1) * 16)
                    for c in range(3):
                        tile = [grads[c, d, rows, at] for d in range(3)]
                        for n in range(4):
                            f = fields[n]
                            value = f[0] * tile[0] + f[1] * tile[1] + f[2] * tile[2]
                            hold[
                                n * MODES + k * 16 : n * MODES + (k + 1) * 16,
                                c * CUBE + b * LANES : c * CUBE + (b + 1) * LANES,
                            ] = value
            result = lax.dot_general(
                tests[...], hold[...], (((1,), (1,)), ((), ())), preferred_element_type=jnp.float32
            )
            for a in range(2):
                block = result[:, a * LANES : (a + 1) * LANES]
                out_ref[2 * pair + a] = block.reshape(8, 8, LANES).astype(out_ref.dtype)


def local_tensor(core, fields, wq, block_rs, along_t, interpret=False):
    shape = (OWNERS, 8, 8, LANES)
    vmem = pl.BlockSpec(memory_space=pltpu.VMEM)
    return pl.pallas_call(
        tensor_kernel,
        out_shape=(
            jax.ShapeDtypeStruct(shape, jnp.bfloat16),
            jax.ShapeDtypeStruct(shape, jnp.bfloat16),
        ),
        in_specs=[pl.BlockSpec(memory_space=pltpu.SMEM), vmem, vmem, vmem, vmem],
        out_specs=(vmem, vmem),
        scratch_shapes=[
            pltpu.VMEM((3, MODES, CUBE), jnp.float32),
            pltpu.VMEM((3, 3, MODES, CUBE), jnp.bfloat16),
            pltpu.VMEM((MODES, 3 * CUBE), jnp.bfloat16),
            pltpu.VMEM((2, 4 * MODES, 3 * CUBE), jnp.bfloat16),
        ],
        compiler_params=pltpu.CompilerParams(vmem_limit_bytes=16 * 2**20),
        cost_estimate=pl.CostEstimate(flops=4 * 10**9, bytes_accessed=2**21, transcendentals=0),
        interpret=interpret,
        name="tensor",
    )(core, fields, wq, block_rs, along_t)


TEST = ("y_hi", "x")
REST = ("y_lo", "z", "y_hi", "x")


def body(mode_fields, elem_type, type_scales):
    bf16 = jnp.bfloat16
    block_rs, along_t, cube_weights = lobatto_tables(Q)
    block_rs = jnp.asarray(block_rs).astype(bf16)
    along_t = jnp.asarray(along_t).astype(bf16)
    total_points = CUBE * 256
    mine = lax.axis_index(TEST)
    kind = jnp.sum(jnp.where(jnp.arange(8, dtype=jnp.int32) == mine, elem_type, 0))
    picks = (jnp.arange(type_scales.shape[0], dtype=jnp.int32) == kind).astype(jnp.float32)
    scales = jnp.sum(picks[:, None] * type_scales, axis=0)
    wq = scales[:, None] * (jnp.asarray(cube_weights)[None, :] / jnp.prod(scales))
    pieces = mode_fields.reshape(8, 3, 8, CUBE).transpose(2, 1, 0, 3)
    fields = lax.all_to_all(pieces, TEST, 0, 0, tiled=True)
    core = lax.axis_index("core").astype(jnp.int32).reshape(1)
    send, own = local_tensor(core, fields, wq, block_rs, along_t)
    other = lax.ppermute(send, "core", [(0, 1), (1, 0)])
    both = (own.astype(jnp.float32) + other.astype(jnp.float32)).astype(bf16)
    chunks = lax.all_to_all(both.reshape(128, 8, LANES), REST, 0, 0, tiled=True)
    summed = jnp.sum(chunks.astype(jnp.float32), axis=0)
    return (summed * float(total_points) ** (-0.5)).reshape(8, 2, MODES)


def solution(mesh):
    split = Mesh(
        mesh.devices.reshape(2, 8, 2, 2, 4), ("y_lo", "z", "core", "y_hi", "x")
    )
    elem = ("y_lo", "z", "core")
    placed = (P(TEST, None, elem), P(elem), P())
    return jax.shard_map(
        body, mesh=split, in_specs=placed, out_specs=P(TEST, elem, None), check_vma=False
    )
```

```python
import functools

import jax
import jax.numpy as jnp
import numpy as np
from jax import lax
from jax.experimental import pallas as pl
from jax.experimental.pallas import tpu as pltpu
from jax.sharding import Mesh, PartitionSpec as P

Q = 8
CUBE = Q**3
MODES = 64
LANES = 128
OWNERS = 16
TEST = ("y_hi", "x")


def legendre_top(points, degree):
    before = points * 0.0 + 1.0
    current = points
    for order in range(2, degree + 1):
        following = ((2 * order - 1) * points * current - (order - 1) * before) / order
        before = current
        current = following
    return (current, before)


def lobatto_tables(order_points):
    degree = order_points - 1
    lobatto_nodes = np.cos(np.pi * np.arange(degree + 1) / degree)
    for sweep in range(100):
        top, lower = legendre_top(lobatto_nodes, degree)
        lobatto_nodes = lobatto_nodes - (lobatto_nodes * top - lower) / ((degree + 1) * top)
    lobatto_nodes = lobatto_nodes[::-1].copy()
    lobatto_nodes[0] = -1.0
    lobatto_nodes[-1] = 1.0
    values, unused = legendre_top(lobatto_nodes, degree)
    weights = 2.0 / (degree * (degree + 1) * values**2)
    identity = np.eye(order_points)
    distance = lobatto_nodes[:, None] - lobatto_nodes[None, :]
    spacing = np.where(identity > 0, 1.0, distance)
    derivative = np.where(identity > 0, 0.0, values[:, None] / values[None, :] / spacing)
    corner = degree * (degree + 1) / 4.0
    ends = np.concatenate([[-corner], np.zeros(degree - 1), [corner]])
    derivative = derivative + identity * ends[None, :]
    block_r = np.kron(np.eye(16), derivative)
    block_s = np.kron(np.eye(2), np.kron(derivative, identity))
    block_rs = np.concatenate([block_r.T, block_s.T], axis=1)
    along_t = np.kron(derivative, np.eye(order_points * order_points))
    cube_weights = np.kron(weights, np.kron(weights, weights))
    return (
        block_rs.astype(np.float32),
        along_t.T.astype(np.float32),
        cube_weights.astype(np.float32),
    )


def tensor_kernel(
    kinds_ref, types_ref, weights_ref, x_ref, rs_ref, tt_ref, send_ref, own_ref, wide, grads, tests
):
    bf16 = jnp.bfloat16
    f32 = jnp.float32
    blocks = CUBE // LANES
    core = lax.axis_index("core")
    mine = lax.axis_index(TEST)
    kinds = kinds_ref[...]
    here = lax.broadcasted_iota(jnp.int32, kinds.shape, 1) == mine
    kind = jnp.sum(jnp.where(here, kinds.astype(f32), 0.0), axis=1, keepdims=True)
    table = types_ref[...]
    picked = lax.broadcasted_iota(jnp.int32, table.shape, 0).astype(f32) == kind
    scales = jnp.sum(jnp.where(picked, table, 0.0), axis=0, keepdims=True)
    along = [scales[:, d : d + 1] for d in range(3)]
    quad = weights_ref[...] / (along[0] * along[1] * along[2])
    high = (lax.broadcasted_iota(jnp.int32, (MODES, CUBE), 0) & 2) != 0
    swap = jnp.broadcast_to(core, (MODES, CUBE)) != 0
    narrow = []
    for c in range(3):
        rows = jnp.concatenate([x_ref[s, c].astype(f32) for s in range(8)], axis=0)
        turned = jnp.where(high, pltpu.roll(rows, 2, 0), pltpu.roll(rows, MODES - 2, 0))
        turned = jnp.where(swap, turned, rows)
        weighted = rows * quad
        upper = weighted.astype(bf16)
        lower = (weighted - upper.astype(f32)).astype(bf16)
        for b in range(blocks):
            at = slice(b * LANES, (b + 1) * LANES)
            wide[c, b] = turned[:, at]
            tests[c * blocks + b, :MODES] = upper[:, at]
            tests[c * blocks + b, MODES:] = lower[:, at]
        narrow.append(rows.astype(bf16))
    panel = jnp.concatenate(narrow, axis=0)
    along_t = jnp.dot(panel, tt_ref[...], preferred_element_type=f32)
    for b in range(blocks):
        at = slice(b * LANES, (b + 1) * LANES)
        along_rs = jnp.dot(panel[:, at], rs_ref[...], preferred_element_type=f32)
        parts = (along_rs[:, :LANES], along_rs[:, LANES:], along_t[:, at])
        for d in range(3):
            scaled = (parts[d] * along[d]).astype(bf16)
            for c in range(3):
                grads[c, d, b] = scaled[c * MODES : (c + 1) * MODES]
    for slot, out_ref in ((0, send_ref), (1, own_ref)):
        for pair in range(OWNERS // 2):
            made = {}
            trial = [
                4 * (2 * pair + a) + 2 * (1 - slot) + jj for a in range(2) for jj in range(2)
            ]
            for b in range(blocks):
                fields = [
                    [
                        jnp.broadcast_to(wide[d, b, j : j + 1], (16, LANES)).astype(bf16)
                        for d in range(3)
                    ]
                    for j in trial
                ]
                for k in range(MODES // 16):
                    rows = slice(k * 16, (k + 1) * 16)
                    for c in range(3):
                        tile = [grads[c, d, b, rows] for d in range(3)]
                        for n in range(4):
                            f = fields[n]
                            value = f[0] * tile[0] + f[1] * tile[1] + f[2] * tile[2]
                            made[c * blocks + b, n, k] = value
            left = jnp.concatenate([tests[n] for n in range(3 * blocks)], axis=1)
            right = jnp.concatenate(
                [
                    jnp.concatenate(
                        [made[m, n, k] for n in range(4) for k in range(MODES // 16)], axis=0
                    )
                    for m in range(3 * blocks)
                ],
                axis=1,
            )
            both = lax.dot_general(
                left, right, (((1,), (1,)), ((), ())), preferred_element_type=f32
            )
            result = both[:MODES] + both[MODES:]
            for a in range(2):
                block = result[:, a * LANES : (a + 1) * LANES]
                out_ref[2 * pair + a] = block.reshape(8, 8, LANES).astype(out_ref.dtype)


def local_tensor(kinds, types, weights, fields, block_rs, along_t, interpret=False):
    shape = (OWNERS, 8, 8, LANES)
    blocks = CUBE // LANES
    vmem = pl.BlockSpec(memory_space=pltpu.VMEM)
    return pl.pallas_call(
        tensor_kernel,
        out_shape=(
            jax.ShapeDtypeStruct(shape, jnp.bfloat16),
            jax.ShapeDtypeStruct(shape, jnp.float32),
        ),
        in_specs=[vmem] * 6,
        out_specs=(vmem, vmem),
        scratch_shapes=[
            pltpu.VMEM((3, blocks, MODES, LANES), jnp.float32),
            pltpu.VMEM((3, 3, blocks, MODES, LANES), jnp.bfloat16),
            pltpu.VMEM((3 * blocks, 2 * MODES, LANES), jnp.bfloat16),
        ],
        compiler_params=pltpu.CompilerParams(vmem_limit_bytes=16 * 2**20),
        cost_estimate=pl.CostEstimate(flops=4 * 10**9, bytes_accessed=2**21, transcendentals=0),
        interpret=interpret,
        name="tensor",
    )(kinds, types, weights, fields, block_rs, along_t)


REST = ("y_lo", "z", "y_hi", "x")


def body(mode_fields, elem_type, type_scales):
    bf16 = jnp.bfloat16
    block_rs, along_t, cube_weights = lobatto_tables(Q)
    block_rs = jnp.asarray(block_rs).astype(bf16)
    along_t = jnp.asarray(along_t).astype(bf16)
    total_points = CUBE * 256
    pieces = mode_fields.reshape(8, 3, 8, CUBE).transpose(2, 1, 0, 3)
    fields = lax.all_to_all(pieces, TEST, 0, 0, tiled=True)
    send, own = local_tensor(
        elem_type.reshape(1, 8), type_scales, jnp.asarray(cube_weights)[None], fields, block_rs, along_t
    )
    other = lax.ppermute(send, "core", [(0, 1), (1, 0)])
    both = (own + other.astype(jnp.float32)).astype(bf16)
    chunks = lax.all_to_all(both.reshape(128, 8, LANES), REST, 0, 0, tiled=True)
    summed = jnp.sum(chunks.astype(jnp.float32), axis=0)
    return (summed * float(total_points) ** (-0.5)).reshape(8, 2, MODES)


def solution(mesh):
    split = Mesh(
        mesh.devices.reshape(2, 8, 2, 2, 4), ("y_lo", "z", "core", "y_hi", "x")
    )
    elem = ("y_lo", "z", "core")
    placed = (P(TEST, None, elem), P(elem), P())
    return jax.shard_map(
        body, mesh=split, in_specs=placed, out_specs=P(TEST, elem, None), check_vma=False
    )
```

```python
import functools

import jax
import jax.numpy as jnp
import numpy as np
from jax import lax
from jax.experimental import pallas as pl
from jax.experimental.pallas import tpu as pltpu
from jax.sharding import Mesh, PartitionSpec as P

Q = 8
CUBE = Q**3
MODES = 64
LANES = 128
OWNERS = 16
TEST = ("y_hi", "x")


def legendre_top(points, degree):
    before = points * 0.0 + 1.0
    current = points
    for order in range(2, degree + 1):
        following = ((2 * order - 1) * points * current - (order - 1) * before) / order
        before = current
        current = following
    return (current, before)


def lobatto_tables(order_points):
    degree = order_points - 1
    lobatto_nodes = np.cos(np.pi * np.arange(degree + 1) / degree)
    for sweep in range(100):
        top, lower = legendre_top(lobatto_nodes, degree)
        lobatto_nodes = lobatto_nodes - (lobatto_nodes * top - lower) / ((degree + 1) * top)
    lobatto_nodes = lobatto_nodes[::-1].copy()
    lobatto_nodes[0] = -1.0
    lobatto_nodes[-1] = 1.0
    values, unused = legendre_top(lobatto_nodes, degree)
    weights = 2.0 / (degree * (degree + 1) * values**2)
    identity = np.eye(order_points)
    distance = lobatto_nodes[:, None] - lobatto_nodes[None, :]
    spacing = np.where(identity > 0, 1.0, distance)
    derivative = np.where(identity > 0, 0.0, values[:, None] / values[None, :] / spacing)
    corner = degree * (degree + 1) / 4.0
    ends = np.concatenate([[-corner], np.zeros(degree - 1), [corner]])
    derivative = derivative + identity * ends[None, :]
    block_r = np.kron(np.eye(16), derivative)
    block_s = np.kron(np.eye(2), np.kron(derivative, identity))
    block_rs = np.concatenate([block_r.T, block_s.T], axis=1)
    along_t = np.kron(derivative, np.eye(order_points * order_points))
    cube_weights = np.kron(weights, np.kron(weights, weights))
    return (
        block_rs.astype(np.float32),
        along_t.T.astype(np.float32),
        cube_weights.astype(np.float32),
    )


def contract(slot, out_ref, wide, grads, tests):
    bf16 = jnp.bfloat16
    f32 = jnp.float32
    blocks = CUBE // LANES
    for pair in range(OWNERS // 2):
        made = {}
        trial = [4 * (2 * pair + a) + 2 * (1 - slot) + jj for a in range(2) for jj in range(2)]
        for b in range(blocks):
            fields = [
                [
                    jnp.broadcast_to(wide[d, b, j : j + 1], (16, LANES)).astype(bf16)
                    for d in range(3)
                ]
                for j in trial
            ]
            for k in range(MODES // 16):
                rows = slice(k * 16, (k + 1) * 16)
                for c in range(3):
                    tile = [grads[c, d, b, rows] for d in range(3)]
                    for n in range(4):
                        f = fields[n]
                        value = f[0] * tile[0] + f[1] * tile[1] + f[2] * tile[2]
                        made[c * blocks + b, n, k] = value
        left = jnp.concatenate([tests[n] for n in range(3 * blocks)], axis=1)
        right = jnp.concatenate(
            [
                jnp.concatenate(
                    [made[m, n, k] for n in range(4) for k in range(MODES // 16)], axis=0
                )
                for m in range(3 * blocks)
            ],
            axis=1,
        )
        both = lax.dot_general(left, right, (((1,), (1,)), ((), ())), preferred_element_type=f32)
        result = both[:MODES] + both[MODES:]
        for a in range(2):
            block = result[:, a * LANES : (a + 1) * LANES]
            out_ref[2 * pair + a] = block.reshape(8, 8, LANES).astype(out_ref.dtype)


def first_kernel(kinds_ref, types_ref, weights_ref, x_ref, rs_ref, tt_ref, send_ref, wide, grads, tests):
    bf16 = jnp.bfloat16
    f32 = jnp.float32
    blocks = CUBE // LANES
    core = lax.axis_index("core")
    kinds = kinds_ref[...].reshape(1, 8)
    here = lax.broadcasted_iota(jnp.int32, (1, 8), 1) == lax.axis_index(TEST)
    kind = jnp.sum(jnp.where(here, kinds.astype(f32), 0.0), axis=1, keepdims=True)
    picked = lax.broadcasted_iota(jnp.int32, (4, 3), 0).astype(f32) == kind
    scales = jnp.sum(jnp.where(picked, types_ref[...], 0.0), axis=0, keepdims=True)
    along = [scales[:, d : d + 1] for d in range(3)]
    quad = weights_ref[...] / (along[0] * along[1] * along[2])
    high = (lax.broadcasted_iota(jnp.int32, (MODES, CUBE), 0) & 2) != 0
    swap = jnp.broadcast_to(core, (MODES, CUBE)) != 0
    narrow = []
    for c in range(3):
        rows = jnp.concatenate([x_ref[s, c].astype(f32) for s in range(8)], axis=0)
        turned = jnp.where(high, pltpu.roll(rows, 2, 0), pltpu.roll(rows, MODES - 2, 0))
        turned = jnp.where(swap, turned, rows)
        weighted = rows * quad
        upper = weighted.astype(bf16)
        lower = (weighted - upper.astype(f32)).astype(bf16)
        for b in range(blocks):
            at = slice(b * LANES, (b + 1) * LANES)
            wide[c, b] = turned[:, at]
            tests[c * blocks + b, :MODES] = upper[:, at]
            tests[c * blocks + b, MODES:] = lower[:, at]
        narrow.append(rows.astype(bf16))
    panel = jnp.concatenate(narrow, axis=0)
    along_t = jnp.dot(panel, tt_ref[...], preferred_element_type=f32)
    for b in range(blocks):
        at = slice(b * LANES, (b + 1) * LANES)
        along_rs = jnp.dot(panel[:, at], rs_ref[...], preferred_element_type=f32)
        parts = (along_rs[:, :LANES], along_rs[:, LANES:], along_t[:, at])
        for d in range(3):
            scaled = (parts[d] * along[d]).astype(bf16)
            for c in range(3):
                grads[c, d, b] = scaled[c * MODES : (c + 1) * MODES]
    contract(0, send_ref, wide, grads, tests)


def second_kernel(wide, grads, tests, own_ref):
    contract(1, own_ref, wide, grads, tests)


SHAPE = (OWNERS, 8, 8, LANES)


def first_half(kinds, types, weights, fields, block_rs, along_t):
    blocks = CUBE // LANES
    vmem = pl.BlockSpec(memory_space=pltpu.VMEM)
    return pl.pallas_call(
        first_kernel,
        out_shape=(
            jax.ShapeDtypeStruct(SHAPE, jnp.bfloat16),
            jax.ShapeDtypeStruct((3, blocks, MODES, LANES), jnp.float32),
            jax.ShapeDtypeStruct((3, 3, blocks, MODES, LANES), jnp.bfloat16),
            jax.ShapeDtypeStruct((3 * blocks, 2 * MODES, LANES), jnp.bfloat16),
        ),
        in_specs=[vmem] * 6,
        out_specs=(vmem,) * 4,
        compiler_params=pltpu.CompilerParams(vmem_limit_bytes=16 * 2**20),
        cost_estimate=pl.CostEstimate(flops=3 * 10**9, bytes_accessed=2**21, transcendentals=0),
        name="first",
    )(kinds, types, weights, fields, block_rs, along_t)


def second_half(wide, grads, tests):
    vmem = pl.BlockSpec(memory_space=pltpu.VMEM)
    return pl.pallas_call(
        second_kernel,
        out_shape=jax.ShapeDtypeStruct(SHAPE, jnp.float32),
        in_specs=[vmem] * 3,
        out_specs=vmem,
        compiler_params=pltpu.CompilerParams(vmem_limit_bytes=16 * 2**20),
        cost_estimate=pl.CostEstimate(flops=2 * 10**9, bytes_accessed=2**21, transcendentals=0),
        name="second",
    )(wide, grads, tests)


REST = ("y_lo", "z", "y_hi", "x")


def body(mode_fields, elem_type, type_scales):
    bf16 = jnp.bfloat16
    block_rs, along_t, cube_weights = lobatto_tables(Q)
    block_rs = jnp.asarray(block_rs).astype(bf16)
    along_t = jnp.asarray(along_t).astype(bf16)
    total_points = CUBE * 256
    pieces = mode_fields.reshape(8, 3, 8, CUBE).transpose(2, 1, 0, 3)
    fields = lax.all_to_all(pieces, TEST, 0, 0, tiled=True)
    send, wide, grads, tests = first_half(
        elem_type, type_scales, jnp.asarray(cube_weights)[None], fields, block_rs, along_t
    )
    other = lax.ppermute(send, "core", [(0, 1), (1, 0)])
    own = second_half(wide, grads, tests)
    both = (own + other.astype(jnp.float32)).astype(bf16)
    chunks = lax.all_to_all(both.reshape(128, 8, LANES), REST, 0, 0, tiled=True)
    summed = jnp.sum(chunks.astype(jnp.float32), axis=0)
    return (summed * float(total_points) ** (-0.5)).reshape(8, 2, MODES)


def solution(mesh):
    split = Mesh(
        mesh.devices.reshape(2, 8, 2, 2, 4), ("y_lo", "z", "core", "y_hi", "x")
    )
    elem = ("y_lo", "z", "core")
    placed = (P(TEST, None, elem), P(elem), P())
    return jax.shard_map(
        body, mesh=split, in_specs=placed, out_specs=P(TEST, elem, None), check_vma=False
    )
```

```python
import functools

import jax
import jax.numpy as jnp
import numpy as np
from jax import lax
from jax.experimental import pallas as pl
from jax.experimental.pallas import tpu as pltpu
from jax.sharding import Mesh, PartitionSpec as P

Q = 8
CUBE = Q**3
MODES = 64
LANES = 128
OWNERS = 16
TEST = ("y_hi", "x")


def legendre_top(points, degree):
    before = points * 0.0 + 1.0
    current = points
    for order in range(2, degree + 1):
        following = ((2 * order - 1) * points * current - (order - 1) * before) / order
        before = current
        current = following
    return (current, before)


def lobatto_tables(order_points):
    degree = order_points - 1
    lobatto_nodes = np.cos(np.pi * np.arange(degree + 1) / degree)
    for sweep in range(100):
        top, lower = legendre_top(lobatto_nodes, degree)
        lobatto_nodes = lobatto_nodes - (lobatto_nodes * top - lower) / ((degree + 1) * top)
    lobatto_nodes = lobatto_nodes[::-1].copy()
    lobatto_nodes[0] = -1.0
    lobatto_nodes[-1] = 1.0
    values, unused = legendre_top(lobatto_nodes, degree)
    weights = 2.0 / (degree * (degree + 1) * values**2)
    identity = np.eye(order_points)
    distance = lobatto_nodes[:, None] - lobatto_nodes[None, :]
    spacing = np.where(identity > 0, 1.0, distance)
    derivative = np.where(identity > 0, 0.0, values[:, None] / values[None, :] / spacing)
    corner = degree * (degree + 1) / 4.0
    ends = np.concatenate([[-corner], np.zeros(degree - 1), [corner]])
    derivative = derivative + identity * ends[None, :]
    block_r = np.kron(np.eye(16), derivative)
    block_s = np.kron(np.eye(2), np.kron(derivative, identity))
    block_rs = np.concatenate([block_r.T, block_s.T], axis=1)
    along_t = np.kron(derivative, np.eye(order_points * order_points))
    cube_weights = np.kron(weights, np.kron(weights, weights))
    return (
        block_rs.astype(np.float32),
        along_t.T.astype(np.float32),
        cube_weights.astype(np.float32),
    )


def contract(slot, out_ref, wide, grads, tests):
    bf16 = jnp.bfloat16
    f32 = jnp.float32
    blocks = CUBE // LANES
    for pair in range(OWNERS // 2):
        made = {}
        trial = [4 * (2 * pair + a) + 2 * (1 - slot) + jj for a in range(2) for jj in range(2)]
        for b in range(blocks):
            fields = [
                [
                    jnp.broadcast_to(wide[d, b, j : j + 1], (16, LANES)).astype(bf16)
                    for d in range(3)
                ]
                for j in trial
            ]
            for k in range(MODES // 16):
                rows = slice(k * 16, (k + 1) * 16)
                for c in range(3):
                    tile = [grads[c, d, b, rows] for d in range(3)]
                    for n in range(4):
                        f = fields[n]
                        value = f[0] * tile[0] + f[1] * tile[1] + f[2] * tile[2]
                        made[c * blocks + b, n, k] = value
        left = jnp.concatenate([tests[n] for n in range(3 * blocks)], axis=1)
        right = jnp.concatenate(
            [
                jnp.concatenate(
                    [made[m, n, k] for n in range(4) for k in range(MODES // 16)], axis=0
                )
                for m in range(3 * blocks)
            ],
            axis=1,
        )
        result = lax.dot_general(left, right, (((1,), (1,)), ((), ())), preferred_element_type=f32)
        for a in range(2):
            block = result[:, a * LANES : (a + 1) * LANES]
            out_ref[2 * pair + a] = block.reshape(8, 8, LANES).astype(out_ref.dtype)


def first_kernel(kinds_ref, types_ref, weights_ref, x_ref, rs_ref, tt_ref, send_ref, wide, grads, tests):
    bf16 = jnp.bfloat16
    f32 = jnp.float32
    blocks = CUBE // LANES
    core = lax.axis_index("core")
    kinds = kinds_ref[...].reshape(1, 8)
    here = lax.broadcasted_iota(jnp.int32, (1, 8), 1) == lax.axis_index(TEST)
    kind = jnp.sum(jnp.where(here, kinds.astype(f32), 0.0), axis=1, keepdims=True)
    picked = lax.broadcasted_iota(jnp.int32, (4, 3), 0).astype(f32) == kind
    scales = jnp.sum(jnp.where(picked, types_ref[...], 0.0), axis=0, keepdims=True)
    along = [scales[:, d : d + 1] for d in range(3)]
    quad = weights_ref[...] / (along[0] * along[1] * along[2])
    high = (lax.broadcasted_iota(jnp.int32, (MODES, CUBE), 0) & 2) != 0
    swap = jnp.broadcast_to(core, (MODES, CUBE)) != 0
    narrow = []
    for c in range(3):
        rows = jnp.concatenate([x_ref[s, c].astype(f32) for s in range(8)], axis=0)
        turned = jnp.where(high, pltpu.roll(rows, 2, 0), pltpu.roll(rows, MODES - 2, 0))
        turned = jnp.where(swap, turned, rows)
        weighted = (rows * quad).astype(bf16)
        for b in range(blocks):
            at = slice(b * LANES, (b + 1) * LANES)
            wide[c, b] = turned[:, at]
            tests[c * blocks + b] = weighted[:, at]
        narrow.append(rows.astype(bf16))
    panel = jnp.concatenate(narrow, axis=0)
    along_t = jnp.dot(panel, tt_ref[...], preferred_element_type=f32)
    for b in range(blocks):
        at = slice(b * LANES, (b + 1) * LANES)
        along_rs = jnp.dot(panel[:, at], rs_ref[...], preferred_element_type=f32)
        parts = (along_rs[:, :LANES], along_rs[:, LANES:], along_t[:, at])
        for d in range(3):
            scaled = (parts[d] * along[d]).astype(bf16)
            for c in range(3):
                grads[c, d, b] = scaled[c * MODES : (c + 1) * MODES]
    contract(0, send_ref, wide, grads, tests)


def second_kernel(wide, grads, tests, own_ref):
    contract(1, own_ref, wide, grads, tests)


SHAPE = (OWNERS, 8, 8, LANES)


def first_half(kinds, types, weights, fields, block_rs, along_t):
    blocks = CUBE // LANES
    vmem = pl.BlockSpec(memory_space=pltpu.VMEM)
    return pl.pallas_call(
        first_kernel,
        out_shape=(
            jax.ShapeDtypeStruct(SHAPE, jnp.float32),
            jax.ShapeDtypeStruct((3, blocks, MODES, LANES), jnp.float32),
            jax.ShapeDtypeStruct((3, 3, blocks, MODES, LANES), jnp.bfloat16),
            jax.ShapeDtypeStruct((3 * blocks, MODES, LANES), jnp.bfloat16),
        ),
        in_specs=[vmem] * 6,
        out_specs=(vmem,) * 4,
        compiler_params=pltpu.CompilerParams(vmem_limit_bytes=16 * 2**20),
        cost_estimate=pl.CostEstimate(flops=3 * 10**9, bytes_accessed=2**21, transcendentals=0),
        name="first",
    )(kinds, types, weights, fields, block_rs, along_t)


def second_half(wide, grads, tests):
    vmem = pl.BlockSpec(memory_space=pltpu.VMEM)
    return pl.pallas_call(
        second_kernel,
        out_shape=jax.ShapeDtypeStruct(SHAPE, jnp.float32),
        in_specs=[vmem] * 3,
        out_specs=vmem,
        compiler_params=pltpu.CompilerParams(vmem_limit_bytes=16 * 2**20),
        cost_estimate=pl.CostEstimate(flops=2 * 10**9, bytes_accessed=2**21, transcendentals=0),
        name="second",
    )(wide, grads, tests)


REST = ("y_lo", "z", "y_hi", "x")


def body(mode_fields, elem_type, type_scales):
    bf16 = jnp.bfloat16
    block_rs, along_t, cube_weights = lobatto_tables(Q)
    block_rs = jnp.asarray(block_rs).astype(bf16)
    along_t = jnp.asarray(along_t).astype(bf16)
    total_points = CUBE * 256
    pieces = mode_fields.reshape(8, 3, 8, CUBE).transpose(2, 1, 0, 3)
    fields = lax.all_to_all(pieces, TEST, 0, 0, tiled=True)
    send, wide, grads, tests = first_half(
        elem_type, type_scales, jnp.asarray(cube_weights)[None], fields, block_rs, along_t
    )
    other = lax.ppermute(send, "core", [(0, 1), (1, 0)])
    own = second_half(wide, grads, tests)
    both = (own + other.astype(jnp.float32)).astype(bf16)
    chunks = lax.all_to_all(both.reshape(128, 8, LANES), REST, 0, 0, tiled=True)
    summed = jnp.sum(chunks.astype(jnp.float32), axis=0)
    return (summed * float(total_points) ** (-0.5)).reshape(8, 2, MODES)


def solution(mesh):
    split = Mesh(
        mesh.devices.reshape(2, 8, 2, 2, 4), ("y_lo", "z", "core", "y_hi", "x")
    )
    elem = ("y_lo", "z", "core")
    placed = (P(TEST, None, elem), P(elem), P())
    return jax.shard_map(
        body, mesh=split, in_specs=placed, out_specs=P(TEST, elem, None), check_vma=False
    )
```

```python
import functools

import jax
import jax.numpy as jnp
import numpy as np
from jax import lax
from jax.experimental import pallas as pl
from jax.experimental.pallas import tpu as pltpu
from jax.sharding import Mesh, PartitionSpec as P

Q = 8
CUBE = Q**3
MODES = 64
LANES = 128
OWNERS = 16
TEST = ("y_hi", "x")


def legendre_top(points, degree):
    before = points * 0.0 + 1.0
    current = points
    for order in range(2, degree + 1):
        following = ((2 * order - 1) * points * current - (order - 1) * before) / order
        before = current
        current = following
    return (current, before)


def lobatto_tables(order_points):
    degree = order_points - 1
    lobatto_nodes = np.cos(np.pi * np.arange(degree + 1) / degree)
    for sweep in range(100):
        top, lower = legendre_top(lobatto_nodes, degree)
        lobatto_nodes = lobatto_nodes - (lobatto_nodes * top - lower) / ((degree + 1) * top)
    lobatto_nodes = lobatto_nodes[::-1].copy()
    lobatto_nodes[0] = -1.0
    lobatto_nodes[-1] = 1.0
    values, unused = legendre_top(lobatto_nodes, degree)
    weights = 2.0 / (degree * (degree + 1) * values**2)
    identity = np.eye(order_points)
    distance = lobatto_nodes[:, None] - lobatto_nodes[None, :]
    spacing = np.where(identity > 0, 1.0, distance)
    derivative = np.where(identity > 0, 0.0, values[:, None] / values[None, :] / spacing)
    corner = degree * (degree + 1) / 4.0
    ends = np.concatenate([[-corner], np.zeros(degree - 1), [corner]])
    derivative = derivative + identity * ends[None, :]
    block_r = np.kron(np.eye(16), derivative)
    block_s = np.kron(np.eye(2), np.kron(derivative, identity))
    block_rs = np.concatenate([block_r.T, block_s.T], axis=1)
    along_t = np.kron(derivative, np.eye(order_points * order_points))
    cube_weights = np.kron(weights, np.kron(weights, weights))
    return (
        block_rs.astype(np.float32),
        along_t.T.astype(np.float32),
        cube_weights.astype(np.float32),
    )


def contract(slot, out_ref, wide, grads, tests):
    bf16 = jnp.bfloat16
    f32 = jnp.float32
    blocks = CUBE // LANES
    for pair in range(OWNERS // 2):
        made = {}
        trial = [4 * (2 * pair + a) + 2 * (1 - slot) + jj for a in range(2) for jj in range(2)]
        for b in range(blocks):
            fields = [
                [
                    jnp.broadcast_to(wide[d, b, j : j + 1], (16, LANES)).astype(bf16)
                    for d in range(3)
                ]
                for j in trial
            ]
            for k in range(MODES // 16):
                rows = slice(k * 16, (k + 1) * 16)
                for c in range(3):
                    tile = [grads[c, d, b, rows] for d in range(3)]
                    for n in range(4):
                        f = fields[n]
                        value = f[0] * tile[0] + f[1] * tile[1] + f[2] * tile[2]
                        made[c * blocks + b, n, k] = value
        left = jnp.concatenate([tests[n] for n in range(3 * blocks)], axis=1)
        right = jnp.concatenate(
            [
                jnp.concatenate(
                    [made[m, n, k] for n in range(4) for k in range(MODES // 16)], axis=0
                )
                for m in range(3 * blocks)
            ],
            axis=1,
        )
        result = lax.dot_general(left, right, (((1,), (1,)), ((), ())), preferred_element_type=f32)
        for a in range(2):
            block = result[:, a * LANES : (a + 1) * LANES]
            out_ref[2 * pair + a] = block.reshape(8, 8, LANES).astype(out_ref.dtype)


def first_kernel(kinds_ref, types_ref, weights_ref, x_ref, rs_ref, tt_ref, send_ref, wide, grads, tests):
    bf16 = jnp.bfloat16
    f32 = jnp.float32
    blocks = CUBE // LANES
    core = lax.axis_index("core")
    kinds = kinds_ref[...].reshape(1, 8)
    here = lax.broadcasted_iota(jnp.int32, (1, 8), 1) == lax.axis_index(TEST)
    kind = jnp.sum(jnp.where(here, kinds.astype(f32), 0.0), axis=1, keepdims=True)
    picked = lax.broadcasted_iota(jnp.int32, (4, 3), 0).astype(f32) == kind
    scales = jnp.sum(jnp.where(picked, types_ref[...], 0.0), axis=0, keepdims=True)
    along = [scales[:, d : d + 1] for d in range(3)]
    quad = weights_ref[...] / (along[0] * along[1] * along[2])
    high = (lax.broadcasted_iota(jnp.int32, (MODES, CUBE), 0) & 2) != 0
    swap = jnp.broadcast_to(core, (MODES, CUBE)) != 0
    narrow = []
    for c in range(3):
        rows = jnp.concatenate([x_ref[s, c].astype(f32) for s in range(8)], axis=0)
        turned = jnp.where(high, pltpu.roll(rows, 2, 0), pltpu.roll(rows, MODES - 2, 0))
        turned = jnp.where(swap, turned, rows)
        weighted = (rows * quad).astype(bf16)
        for b in range(blocks):
            at = slice(b * LANES, (b + 1) * LANES)
            wide[c, b] = turned[:, at]
            tests[c * blocks + b] = weighted[:, at]
        narrow.append(rows.astype(bf16))
    panel = jnp.concatenate(narrow, axis=0)
    along_t = jnp.dot(panel, tt_ref[...], preferred_element_type=f32)
    for b in range(blocks):
        at = slice(b * LANES, (b + 1) * LANES)
        along_rs = jnp.dot(panel[:, at], rs_ref[...], preferred_element_type=f32)
        parts = (along_rs[:, :LANES], along_rs[:, LANES:], along_t[:, at])
        for d in range(3):
            scaled = (parts[d] * along[d]).astype(bf16)
            for c in range(3):
                grads[c, d, b] = scaled[c * MODES : (c + 1) * MODES]
    contract(0, send_ref, wide, grads, tests)


def second_kernel(wide, grads, tests, own_ref):
    contract(1, own_ref, wide, grads, tests)


SHAPE = (OWNERS, 8, 8, LANES)


def first_half(kinds, types, weights, fields, block_rs, along_t):
    blocks = CUBE // LANES
    vmem = pl.BlockSpec(memory_space=pltpu.VMEM)
    return pl.pallas_call(
        first_kernel,
        out_shape=(
            jax.ShapeDtypeStruct(SHAPE, jnp.float32),
            jax.ShapeDtypeStruct((3, blocks, MODES, LANES), jnp.float32),
            jax.ShapeDtypeStruct((3, 3, blocks, MODES, LANES), jnp.bfloat16),
            jax.ShapeDtypeStruct((3 * blocks, MODES, LANES), jnp.bfloat16),
        ),
        in_specs=[vmem] * 6,
        out_specs=(vmem,) * 4,
        compiler_params=pltpu.CompilerParams(vmem_limit_bytes=16 * 2**20),
        cost_estimate=pl.CostEstimate(flops=3 * 10**9, bytes_accessed=2**21, transcendentals=0),
        name="first",
    )(kinds, types, weights, fields, block_rs, along_t)


def second_half(wide, grads, tests):
    vmem = pl.BlockSpec(memory_space=pltpu.VMEM)
    return pl.pallas_call(
        second_kernel,
        out_shape=jax.ShapeDtypeStruct(SHAPE, jnp.float32),
        in_specs=[vmem] * 3,
        out_specs=vmem,
        compiler_params=pltpu.CompilerParams(vmem_limit_bytes=16 * 2**20),
        cost_estimate=pl.CostEstimate(flops=2 * 10**9, bytes_accessed=2**21, transcendentals=0),
        name="second",
    )(wide, grads, tests)


def total_kernel(norm, chunks_ref, out_ref):
    sums = [jnp.zeros((8, LANES), jnp.float32) for _ in range(8)]
    for n in range(8 * OWNERS):
        sums[n % 8] = sums[n % 8] + chunks_ref[n].astype(jnp.float32)
    while len(sums) > 1:
        sums = [sums[n] + sums[n + 1] for n in range(0, len(sums), 2)]
    result = sums[0] * norm
    for jj in range(2):
        out_ref[:, jj, :] = result[:, jj * MODES : (jj + 1) * MODES]


def totalled(chunks, norm):
    vmem = pl.BlockSpec(memory_space=pltpu.VMEM)
    return pl.pallas_call(
        functools.partial(total_kernel, norm),
        out_shape=jax.ShapeDtypeStruct((8, 2, MODES), jnp.float32),
        in_specs=[vmem],
        out_specs=vmem,
        compiler_params=pltpu.CompilerParams(vmem_limit_bytes=8 * 2**20),
        name="total",
    )(chunks)


REST = ("y_lo", "z", "y_hi", "x")


def body(mode_fields, elem_type, type_scales):
    bf16 = jnp.bfloat16
    block_rs, along_t, cube_weights = lobatto_tables(Q)
    block_rs = jnp.asarray(block_rs).astype(bf16)
    along_t = jnp.asarray(along_t).astype(bf16)
    total_points = CUBE * 256
    pieces = mode_fields.reshape(8, 3, 8, CUBE).transpose(2, 1, 0, 3)
    fields = lax.all_to_all(pieces, TEST, 0, 0, tiled=True)
    send, wide, grads, tests = first_half(
        elem_type, type_scales, jnp.asarray(cube_weights)[None], fields, block_rs, along_t
    )
    other = lax.ppermute(send, "core", [(0, 1), (1, 0)])
    own = second_half(wide, grads, tests)
    both = (own + other.astype(jnp.float32)).astype(bf16)
    chunks = lax.all_to_all(both.reshape(128, 8, LANES), REST, 0, 0, tiled=True)
    return totalled(chunks, float(total_points) ** (-0.5))


def solution(mesh):
    split = Mesh(
        mesh.devices.reshape(2, 8, 2, 2, 4), ("y_lo", "z", "core", "y_hi", "x")
    )
    elem = ("y_lo", "z", "core")
    placed = (P(TEST, None, elem), P(elem), P())
    return jax.shard_map(
        body, mesh=split, in_specs=placed, out_specs=P(TEST, elem, None), check_vma=False
    )
```

```python
import functools

import jax
import jax.numpy as jnp
import numpy as np
from jax import lax
from jax.experimental import pallas as pl
from jax.experimental.pallas import tpu as pltpu
from jax.sharding import Mesh, PartitionSpec as P

Q = 8
CUBE = Q**3
MODES = 64
LANES = 128
OWNERS = 16
TEST = ("y_hi", "x")


def legendre_top(points, degree):
    before = points * 0.0 + 1.0
    current = points
    for order in range(2, degree + 1):
        following = ((2 * order - 1) * points * current - (order - 1) * before) / order
        before = current
        current = following
    return (current, before)


def lobatto_tables(order_points):
    degree = order_points - 1
    lobatto_nodes = np.cos(np.pi * np.arange(degree + 1) / degree)
    for sweep in range(100):
        top, lower = legendre_top(lobatto_nodes, degree)
        lobatto_nodes = lobatto_nodes - (lobatto_nodes * top - lower) / ((degree + 1) * top)
    lobatto_nodes = lobatto_nodes[::-1].copy()
    lobatto_nodes[0] = -1.0
    lobatto_nodes[-1] = 1.0
    values, unused = legendre_top(lobatto_nodes, degree)
    weights = 2.0 / (degree * (degree + 1) * values**2)
    identity = np.eye(order_points)
    distance = lobatto_nodes[:, None] - lobatto_nodes[None, :]
    spacing = np.where(identity > 0, 1.0, distance)
    derivative = np.where(identity > 0, 0.0, values[:, None] / values[None, :] / spacing)
    corner = degree * (degree + 1) / 4.0
    ends = np.concatenate([[-corner], np.zeros(degree - 1), [corner]])
    derivative = derivative + identity * ends[None, :]
    block_r = np.kron(np.eye(16), derivative)
    block_s = np.kron(np.eye(2), np.kron(derivative, identity))
    block_rs = np.concatenate([block_r.T, block_s.T], axis=1)
    along_t = np.kron(derivative, np.eye(order_points * order_points))
    cube_weights = np.kron(weights, np.kron(weights, weights))
    return (
        block_rs.astype(np.float32),
        along_t.T.astype(np.float32),
        cube_weights.astype(np.float32),
    )


def contract(slot, out_ref, wide, grads, tests):
    bf16 = jnp.bfloat16
    f32 = jnp.float32
    blocks = CUBE // LANES
    for pair in range(OWNERS // 2):
        made = {}
        trial = [4 * (2 * pair + a) + 2 * (1 - slot) + jj for a in range(2) for jj in range(2)]
        for b in range(blocks):
            fields = [
                [
                    jnp.broadcast_to(wide[d, b, j : j + 1], (16, LANES)).astype(bf16)
                    for d in range(3)
                ]
                for j in trial
            ]
            for k in range(MODES // 16):
                rows = slice(k * 16, (k + 1) * 16)
                for c in range(3):
                    tile = [grads[c, d, b, rows] for d in range(3)]
                    for n in range(4):
                        f = fields[n]
                        value = f[0] * tile[0] + f[1] * tile[1] + f[2] * tile[2]
                        made[c * blocks + b, n, k] = value
        left = jnp.concatenate([tests[n] for n in range(3 * blocks)], axis=1)
        right = jnp.concatenate(
            [
                jnp.concatenate(
                    [made[m, n, k] for n in range(4) for k in range(MODES // 16)], axis=0
                )
                for m in range(3 * blocks)
            ],
            axis=1,
        )
        result = lax.dot_general(left, right, (((1,), (1,)), ((), ())), preferred_element_type=f32)
        for a in range(2):
            block = result[:, a * LANES : (a + 1) * LANES]
            out_ref[2 * pair + a] = block.reshape(8, 8, LANES).astype(out_ref.dtype)


def first_kernel(kinds_ref, types_ref, weights_ref, x_ref, rs_ref, tt_ref, send_ref, wide, grads, tests):
    bf16 = jnp.bfloat16
    f32 = jnp.float32
    blocks = CUBE // LANES
    core = lax.axis_index("core")
    kinds = kinds_ref[...].reshape(1, 8)
    here = lax.broadcasted_iota(jnp.int32, (1, 8), 1) == lax.axis_index(TEST)
    kind = jnp.sum(jnp.where(here, kinds.astype(f32), 0.0), axis=1, keepdims=True)
    picked = lax.broadcasted_iota(jnp.int32, (4, 3), 0).astype(f32) == kind
    scales = jnp.sum(jnp.where(picked, types_ref[...], 0.0), axis=0, keepdims=True)
    along = [scales[:, d : d + 1] for d in range(3)]
    quad = weights_ref[...] / (along[0] * along[1] * along[2])
    high = (lax.broadcasted_iota(jnp.int32, (MODES, CUBE), 0) & 2) != 0
    swap = jnp.broadcast_to(core, (MODES, CUBE)) != 0
    narrow = []
    for c in range(3):
        rows = jnp.concatenate([x_ref[s, c].astype(f32) for s in range(8)], axis=0)
        turned = jnp.where(high, pltpu.roll(rows, 2, 0), pltpu.roll(rows, MODES - 2, 0))
        turned = jnp.where(swap, turned, rows)
        weighted = (rows * quad).astype(bf16)
        for b in range(blocks):
            at = slice(b * LANES, (b + 1) * LANES)
            wide[c, b] = turned[:, at]
            tests[c * blocks + b] = weighted[:, at]
        narrow.append(rows.astype(bf16))
    panel = jnp.concatenate(narrow, axis=0)
    along_t = jnp.dot(panel, tt_ref[...], preferred_element_type=f32)
    for b in range(blocks):
        at = slice(b * LANES, (b + 1) * LANES)
        along_rs = jnp.dot(panel[:, at], rs_ref[...], preferred_element_type=f32)
        parts = (along_rs[:, :LANES], along_rs[:, LANES:], along_t[:, at])
        for d in range(3):
            scaled = (parts[d] * along[d]).astype(bf16)
            for c in range(3):
                grads[c, d, b] = scaled[c * MODES : (c + 1) * MODES]
    contract(0, send_ref, wide, grads, tests)


def second_kernel(wide, grads, tests, own_ref):
    contract(1, own_ref, wide, grads, tests)


SHAPE = (OWNERS, 8, 8, LANES)


def first_half(kinds, types, weights, fields, block_rs, along_t):
    blocks = CUBE // LANES
    vmem = pl.BlockSpec(memory_space=pltpu.VMEM)
    return pl.pallas_call(
        first_kernel,
        out_shape=(
            jax.ShapeDtypeStruct(SHAPE, jnp.bfloat16),
            jax.ShapeDtypeStruct((3, blocks, MODES, LANES), jnp.float32),
            jax.ShapeDtypeStruct((3, 3, blocks, MODES, LANES), jnp.bfloat16),
            jax.ShapeDtypeStruct((3 * blocks, MODES, LANES), jnp.bfloat16),
        ),
        in_specs=[vmem] * 6,
        out_specs=(vmem,) * 4,
        compiler_params=pltpu.CompilerParams(vmem_limit_bytes=16 * 2**20),
        cost_estimate=pl.CostEstimate(flops=3 * 10**9, bytes_accessed=2**21, transcendentals=0),
        name="first",
    )(kinds, types, weights, fields, block_rs, along_t)


def second_half(wide, grads, tests):
    vmem = pl.BlockSpec(memory_space=pltpu.VMEM)
    return pl.pallas_call(
        second_kernel,
        out_shape=jax.ShapeDtypeStruct(SHAPE, jnp.float32),
        in_specs=[vmem] * 3,
        out_specs=vmem,
        compiler_params=pltpu.CompilerParams(vmem_limit_bytes=16 * 2**20),
        cost_estimate=pl.CostEstimate(flops=2 * 10**9, bytes_accessed=2**21, transcendentals=0),
        name="second",
    )(wide, grads, tests)


def total_kernel(norm, chunks_ref, out_ref):
    sums = [jnp.zeros((8, LANES), jnp.float32) for _ in range(8)]
    for n in range(8 * OWNERS):
        sums[n % 8] = sums[n % 8] + chunks_ref[n].astype(jnp.float32)
    while len(sums) > 1:
        sums = [sums[n] + sums[n + 1] for n in range(0, len(sums), 2)]
    result = sums[0] * norm
    for jj in range(2):
        out_ref[:, jj, :] = result[:, jj * MODES : (jj + 1) * MODES]


def totalled(chunks, norm):
    vmem = pl.BlockSpec(memory_space=pltpu.VMEM)
    return pl.pallas_call(
        functools.partial(total_kernel, norm),
        out_shape=jax.ShapeDtypeStruct((8, 2, MODES), jnp.float32),
        in_specs=[vmem],
        out_specs=vmem,
        compiler_params=pltpu.CompilerParams(vmem_limit_bytes=8 * 2**20),
        name="total",
    )(chunks)


REST = ("y_lo", "z", "y_hi", "x")


def body(mode_fields, elem_type, type_scales):
    bf16 = jnp.bfloat16
    block_rs, along_t, cube_weights = lobatto_tables(Q)
    block_rs = jnp.asarray(block_rs).astype(bf16)
    along_t = jnp.asarray(along_t).astype(bf16)
    total_points = CUBE * 256
    pieces = mode_fields.reshape(8, 3, 8, CUBE).transpose(2, 1, 0, 3)
    fields = lax.all_to_all(pieces, TEST, 0, 0, tiled=True)
    send, wide, grads, tests = first_half(
        elem_type, type_scales, jnp.asarray(cube_weights)[None], fields, block_rs, along_t
    )
    other = lax.ppermute(send, "core", [(0, 1), (1, 0)])
    own = second_half(wide, grads, tests)
    both = (own + other.astype(jnp.float32)).astype(bf16)
    chunks = lax.all_to_all(both.reshape(128, 8, LANES), REST, 0, 0, tiled=True)
    return totalled(chunks, float(total_points) ** (-0.5))


def solution(mesh):
    split = Mesh(
        mesh.devices.reshape(2, 8, 2, 2, 4), ("y_lo", "z", "core", "y_hi", "x")
    )
    elem = ("y_lo", "z", "core")
    placed = (P(TEST, None, elem), P(elem), P())
    return jax.shard_map(
        body, mesh=split, in_specs=placed, out_specs=P(TEST, elem, None), check_vma=False
    )
```
